512 devices in a mesh: sweep: 2 (over y), expert: 64 (over z, core), dp: 4 (over x).
Axes of the slice: x: 4, y: 2, z: 32, core: 2. Of those that a mesh axis runs over, the one named last changes fastest.
The devices are a block of a 4x16x32 slice.
Arguments:
- tokens: bfloat16 [65536, 1536], P(('sweep', 'expert', 'dp')), parts along dimension 0, may hold values from -6 to 6
- expert_ids: int32 [65536, 8], P(('sweep', 'expert', 'dp')), parts along dimension 0, may hold values from 0 to 63, all different within a row; in each aligned block of 128 rows (0 to 127, 128 to 255, ...) at most 20 rows name the same one
- gate_weights: float32 [65536, 8], P(('sweep', 'expert', 'dp')), parts along dimension 0, may hold values from 0.1 to 0.6
- expert_in: bfloat16 [128, 1536, 768], P(('sweep', 'expert'), 'dp'), parts along dimension 0, may hold values from -0.15625 to 0.15625
- expert_out: bfloat16 [128, 768, 1536], P(('sweep', 'expert'), None, 'dp'), parts along dimension 0, may hold values from -0.21875 to 0.21875
- shared_in: bfloat16 [3072, 768], P(('sweep', 'dp')), parts along dimension 0, may hold values from -0.15625 to 0.15625
- shared_out: bfloat16 [1536, 1536], P('sweep', 'dp'), parts along dimension 0, may hold values from -0.21875 to 0.21875
Outputs:
- block_out: bfloat16 [65536, 1536], P(('sweep', 'expert', 'dp')), parts along dimension 0
The draws below stay inside these ranges and needn't reach their ends.
There are 2 independent parts, one for each index of `sweep`. The reference program is written for one: setup_inputs(seed, part) draws one part's arguments, and reference() takes and returns one part's arrays. A program takes and returns all parts, laid end to end along the dimension named above; each array names one. Nothing has to cross between parts.
Inputs may be any that keep to these rules, and one draw needn't show every extreme that they name: `expert_ids`: each token names 8 different experts. In each aligned block of 128 tokens (the tokens of one device) no expert is named by more than 20 tokens; some blocks have an expert named by exactly 20.
All inputs are finite; a program needn't handle non-finite values.
Results may differ from the reference program's by a relative error of at most 0.0051.
Values may be sent and summed in bfloat16 or wider, within the bound.
A program may use at most 64 MiB of HBM per device.

```python
import math
import jax
import jax.numpy as jnp
import numpy as np
from jax import lax

D = 1536
FF = 768
EXPERTS = 64
TOPK = 8
TOK_DEV = 128
CAP = 20
TOKENS = 32768


def levels(rng, shape, split, least, top_value):
    def one(position, parts):
        heights = jax.random.uniform(jax.random.fold_in(jax.random.fold_in(rng, 6), position), (parts,), jnp.float32, least / len(split), top_value / len(split))
        return jnp.repeat(jnp.exp(heights), shape[position] // parts).reshape((-1,) + (1,) * (len(shape) - position - 1))

    loudness = one(*split[0])
    for cut in split[1:]:
        loudness = loudness * one(*cut)
    return loudness


def assign_block(key, own, number, rows, amount, top, reach, slope):
    sequence = jax.random.permutation(key, amount)
    heavy_load, usual = load_shares(amount, rows * top, reach, slope, True), load_shares(amount, rows * top, reach, slope, False)
    places = jnp.arange(amount)

    def named(lengths, rotation):
        used = int((lengths > 0).sum())
        fixed = max(1, used // 4)
        moved = fixed + (places - fixed + rotation * (used - fixed)) % max(1, amount - fixed)
        return jnp.zeros((amount,), jnp.int32).at[sequence[jnp.where(places < fixed, places, moved)]].set(jnp.asarray(lengths, jnp.int32))

    lengths = jnp.where(number % 4 == 0, named(heavy_load, number // 4), named(usual, number - number // 4 - 1))
    mixed = jax.random.permutation(jax.random.fold_in(own, 3), amount)
    donor, taker = mixed[0:amount // 2 * 2:2], mixed[1:amount // 2 * 2:2]
    margin = jnp.minimum(lengths[donor] - 1, reach - lengths[taker]) // 2
    margin = jnp.where((donor == sequence[0]) | (taker == sequence[0]) | (lengths[taker] == 0), 0, jnp.maximum(margin, 0))
    moved = jax.random.randint(jax.random.fold_in(own, 4), (amount // 2,), 0, 1 << 20) % (margin + 1)
    lengths = lengths.at[donor].add(-moved).at[taker].add(moved)
    labels = jnp.searchsorted(jnp.cumsum(lengths), jnp.arange(rows * top), side="right").astype(jnp.int32)
    listing = labels.reshape(top, rows).T
    listing = listing[jax.random.permutation(jax.random.fold_in(own, 1), rows)]
    rotation = jax.random.randint(jax.random.fold_in(own, 2), (rows, 1), 0, top)
    return jnp.take_along_axis(listing, (jnp.arange(top)[None, :] + rotation) % top, axis=1)


def load_shares(amount, total, reach, lean, full):
    loads = [(1 << 20) // math.isqrt(grade ** lean) + 1 for grade in range(1, amount + 1)]
    largest = reach if full else min(reach, max(-(-total // amount), total * loads[0] // sum(loads)))
    least = 1 if total - largest >= amount - 1 else 0
    given, spare = [largest] + [least] * (amount - 1), total - largest - least * (amount - 1)
    while spare > 0:
        movable = [i for i in range(1, amount) if given[i] < largest] or [i for i in range(1, amount) if given[i] < reach]
        mass, budget = sum([loads[i] for i in movable]), spare
        for i in movable:
            extra = min(reach - given[i], max(1, budget * loads[i] // mass), spare)
            given[i] = given[i] + extra
            spare = spare - extra
    return np.array(given)


def scatter_about(own_key, dims, scale, limit, cuts=(), kind=jnp.bfloat16):
    level = levels(own_key, dims, cuts, -0.22, 0.18) if cuts else 1.0
    values = jax.random.normal(own_key, dims, jnp.float32) * scale * level
    return jnp.minimum(jnp.maximum(values, -limit), limit).astype(kind)


def setup_inputs(seed: int = 0, part: int = 0) -> dict:
    seeds = jax.random.split(jax.random.key(seed), 8)
    part_splits = jax.random.split(jax.random.fold_in(seeds[7], part), 8)
    tokens = scatter_about(part_splits[0], (TOKENS, D), 1.0, 6.0, ((0, 256),))
    expert_ids_keys = jax.random.split(jax.random.fold_in(part_splits[1], 1), TOKENS // TOK_DEV)
    expert_ids_turns = jax.random.permutation(jax.random.fold_in(part_splits[1], 3), TOKENS // TOK_DEV)
    expert_ids = jax.vmap(lambda own, number: assign_block(jax.random.fold_in(part_splits[1], 2), own, number, TOK_DEV, EXPERTS, TOPK, CAP, 2))(expert_ids_keys, expert_ids_turns).reshape((TOKENS, TOPK))
    gate_weights = jnp.clip(0.1 + 0.5 * jax.random.uniform(part_splits[2], (TOKENS, TOPK), jnp.float32) ** levels(part_splits[2], (TOKENS, TOPK), ((0, 256),), -0.2, 0.2), 0.1, 0.6)
    expert_in = scatter_about(part_splits[3], (EXPERTS, D, FF), D ** -0.5, 0.15625, ((0, 64), (1, 4)))
    expert_out = scatter_about(part_splits[4], (EXPERTS, FF, D), FF ** -0.5, 0.21875, ((0, 64), (2, 4)))
    shared_in = scatter_about(part_splits[5], (D, FF), D ** -0.5, 0.15625, ((0, 4),))
    shared_out = scatter_about(part_splits[6], (FF, D), FF ** -0.5, 0.21875, ((1, 4),))
    return dict(tokens=tokens, expert_ids=expert_ids, gate_weights=gate_weights, expert_in=expert_in, expert_out=expert_out, shared_in=shared_in, shared_out=shared_out)


def layer_norm(tokens):
    values = tokens.astype(jnp.float32)
    center = values - lax.optimization_barrier(jnp.mean(values, axis=-1, keepdims=True))
    spread = lax.optimization_barrier(jnp.mean(center * center, axis=-1, keepdims=True))
    return (center * lax.rsqrt(spread + 1e-06)).astype(jnp.bfloat16)

def reference(tokens, expert_ids, gate_weights, expert_in, expert_out, shared_in, shared_out):
    normed = layer_norm(tokens)
    token_count = tokens.shape[0]
    model_width = tokens.shape[1]
    expert_count = expert_in.shape[0]
    place_count = token_count // TOK_DEV * CAP
    expert_iota = jnp.arange(expert_count, dtype=jnp.int32)
    matches = (expert_ids[:, :, None] == expert_iota[None, None, :]).astype(jnp.int32)
    per_token = lax.optimization_barrier(jnp.sum(matches, axis=1, dtype=jnp.int32))
    earlier = jnp.cumsum(per_token, axis=0, dtype=jnp.int32) - per_token
    slot_of = jnp.take_along_axis(earlier, expert_ids, axis=1).astype(jnp.int32)
    anchors = jnp.broadcast_to(jnp.arange(token_count, dtype=jnp.int32)[:, None], expert_ids.shape)
    slot_table = jnp.full((expert_count, place_count), token_count, jnp.int32)
    slot_table = slot_table.at[expert_ids, slot_of].set(anchors)
    gate_table = jnp.zeros((expert_count, place_count), jnp.float32)
    gate_table = gate_table.at[expert_ids, slot_of].set(gate_weights.astype(jnp.float32))
    padded = jnp.concatenate([normed, jnp.zeros((1, model_width), jnp.bfloat16)], axis=0)

    def expert_step(summed, inputs):
        row_index, gate_rows, weight_in, weight_out = inputs
        gathered = padded[row_index]
        hidden = jax.nn.gelu(jnp.dot(gathered, weight_in, preferred_element_type=jnp.float32)).astype(jnp.bfloat16)
        result = jnp.dot(hidden, weight_out, preferred_element_type=jnp.float32).astype(jnp.bfloat16)
        summed = summed.at[row_index].add(result.astype(jnp.float32) * gate_rows[:, None])
        return (summed, None)
    start_sum = jnp.zeros((token_count + 1, model_width), jnp.float32)
    summed, _ = lax.scan(expert_step, start_sum, (slot_table, gate_table, expert_in, expert_out))
    routed = summed[:token_count]
    shared_hidden = jax.nn.gelu(jnp.dot(normed, shared_in, preferred_element_type=jnp.float32)).astype(jnp.bfloat16)
    shared_result = jnp.dot(shared_hidden, shared_out, preferred_element_type=jnp.float32)
    return (tokens.astype(jnp.float32) + shared_result + routed).astype(jnp.bfloat16)
```

```python
import functools

import jax
import jax.numpy as jnp
from jax import lax
from jax.experimental import pallas as pl
from jax.experimental.pallas import tpu as pltpu
from jax.sharding import PartitionSpec as P

CORES = 2
SLOTS = 32
CHUNKS = 4
FFN_FROM = 7
MESH = pl.DeviceIdType.MESH


def kernel(
    chips, dp, tok_ref, meta_ref, win_ref, wout_ref, sin_ref, sout_ref, out_ref,
    db, mb, st, xb, xs, rc, rs, rb, hb, base, win, wout, sin, sout,
    d_recv, d_send, m_recv, m_send, x_recv, x_send, r_recv, r_send, a_recv, a_send,
    w_recv, w_send, w_loc,
):
    far_r = chips // 2
    far_l = chips - 1 - far_r
    own = far_r - 1
    rows, width = tok_ref.shape
    hidden = win.shape[1]
    part = rows // CHUNKS
    me = lax.axis_index("expert")
    core = lax.rem(me, CORES)
    chip = me // CORES
    right = lax.rem(chip + 1, chips) * CORES + core
    left = lax.rem(chip + chips - 1, chips) * CORES + core
    partner = chip * CORES + (1 - core)
    xi = lax.axis_index("dp")
    x_up, x_down = lax.rem(xi + 1, dp), lax.rem(xi + dp - 1, dp)
    towards = (right, left)

    barrier = pltpu.get_barrier_semaphore()
    for peer in ({"expert": right}, {"expert": left}, {"expert": partner}, {"dp": x_up}, {"dp": x_down}):
        pl.semaphore_signal(barrier, inc=1, device_id=peer, device_id_type=MESH)

    def norm_rows(i, carry):
        rows_i = pl.ds(i * 16, 16)
        values = tok_ref[rows_i, :].astype(jnp.float32)
        center = values - jnp.mean(values, axis=-1, keepdims=True)
        spread = jnp.mean(center * center, axis=-1, keepdims=True)
        db[1, own, rows_i, :] = (center * lax.rsqrt(spread + 1e-06)).astype(jnp.bfloat16)
        return carry

    lax.fori_loop(0, rows // 16, norm_rows, 0)
    mb[1, own] = meta_ref[...]
    pl.semaphore_wait(barrier, 5)

    def piece(k):
        return pl.ds(k * part, part)

    def block_copy(way, source, arrive, k):
        return pltpu.make_async_remote_copy(
            src_ref=db.at[source[0], source[1], piece(k)],
            dst_ref=db.at[way, arrive, piece(k)],
            send_sem=d_send.at[way, arrive],
            recv_sem=d_recv.at[way, arrive, k],
            device_id={"expert": towards[way]},
            device_id_type=MESH,
        )

    def meta_copy(way, source, arrive):
        return pltpu.make_async_remote_copy(
            src_ref=mb.at[source[0], source[1]],
            dst_ref=mb.at[way, arrive],
            send_sem=m_send.at[way, arrive],
            recv_sem=m_recv.at[way, arrive],
            device_id={"expert": towards[way]},
            device_id_type=MESH,
        )

    for way in (0, 1):
        meta_copy(way, (1, own), 0).start()
    for k in range(CHUNKS):
        for way in (0, 1):
            block_copy(way, (1, own), 0, k).start()

    d_part, f_part = win_ref.shape[1], wout_ref.shape[2]

    def region(a, shard):
        if a in (0, 2):
            return (win, sin)[a // 2].at[pl.ds(shard * d_part, d_part), :]
        return (wout, sout)[a // 2].at[:, pl.ds(pl.multiple_of(shard * f_part, 128), f_part)]

    shards = (win_ref.at[0], wout_ref.at[0], sin_ref, sout_ref)

    def weight_copy(a, k):
        shard = lax.rem(xi + dp - k, dp) if a in (0, 2) else lax.rem(xi + k, dp)
        return pltpu.make_async_remote_copy(
            src_ref=shards[a] if k == 0 else region(a, shard),
            dst_ref=region(a, shard),
            send_sem=w_send.at[a, k],
            recv_sem=w_recv.at[a, k],
            device_id={"dp": x_up if a in (0, 2) else x_down},
            device_id_type=MESH,
        )

    def local_copy(a):
        return pltpu.make_async_copy(shards[a], region(a, xi), w_loc.at[a])

    for a in range(4):
        local_copy(a).start()
    for a in (0, 1):
        weight_copy(a, 0).start()

    def slot_copy(way, at):
        return pltpu.make_async_remote_copy(
            src_ref=xs.at[at, way],
            dst_ref=xb.at[at, pl.ds(way * 2 * SLOTS + SLOTS, SLOTS)],
            send_sem=x_send.at[way, at],
            recv_sem=x_recv.at[way, at],
            device_id={"expert": partner},
            device_id_type=MESH,
        )

    def result_copy(way, at):
        return pltpu.make_async_remote_copy(
            src_ref=rs.at[at, way],
            dst_ref=rc.at[at, way, pl.ds(SLOTS, SLOTS)],
            send_sem=r_send.at[way, at],
            recv_sem=r_recv.at[way, at],
            device_id={"expert": partner},
            device_id_type=MESH,
        )

    def sum_copy(way, step, k):
        return pltpu.make_async_remote_copy(
            src_ref=rb.at[way, step, piece(k)],
            dst_ref=rb.at[way, step + 1, piece(k)],
            send_sem=a_send.at[way, step],
            recv_sem=a_recv.at[way, step + 1, k],
            device_id={"expert": towards[1 - way]},
            device_id_type=MESH,
        )

    def gather(way, at):
        ids = mb[way, at, 0:8, :]
        gates = mb[way, at, 8:16, :]
        match, gate = [], []
        for expert in (me, partner):
            hit = ids == expert.astype(jnp.float32)
            match.append(jnp.sum(jnp.where(hit, 1.0, 0.0), axis=0, keepdims=True))
            gate.append(jnp.sum(jnp.where(hit, gates, 0.0), axis=0, keepdims=True))
        both = jnp.concatenate([jnp.broadcast_to(m, (8, rows)) for m in match], axis=0)
        before = lax.broadcasted_iota(jnp.int32, (rows, rows), 0) < lax.broadcasted_iota(jnp.int32, (rows, rows), 1)
        earlier = jnp.dot(
            both.astype(jnp.bfloat16),
            jnp.where(before, 1.0, 0.0).astype(jnp.bfloat16),
            preferred_element_type=jnp.float32,
        )
        slot = jnp.where(both > 0.5, earlier, -1.0)
        row = lax.broadcasted_iota(jnp.int32, (SLOTS, rows), 0).astype(jnp.float32)
        pick, spread = [], []
        for i in (0, 1):
            here = jnp.concatenate([slot[8 * i : 8 * i + 8]] * (SLOTS // 8), axis=0) == row
            pick.append(jnp.where(here, 1.0, 0.0))
            spread.append(jnp.where(here, jnp.broadcast_to(gate[i], (SLOTS, rows)), 0.0))
        picked = jnp.concatenate(pick, axis=0).astype(jnp.bfloat16)
        st[way, at] = jnp.concatenate(spread, axis=0).T.astype(jnp.bfloat16)
        tile = 256
        for n in range(width // tile):
            cols = pl.ds(n * tile, tile)
            got = jnp.dot(picked, db[way, at, :, cols], preferred_element_type=jnp.float32).astype(jnp.bfloat16)
            xb[at, pl.ds(way * 2 * SLOTS, SLOTS), cols] = got[:SLOTS]
            xs[at, way, :, cols] = got[SLOTS:]
        slot_copy(way, at).start()

    def two_dots(source, first, second, store):
        tile = 256
        for n in range(hidden // tile):
            cols = pl.ds(n * tile, tile)
            pre = jnp.dot(source(), first[:, cols], preferred_element_type=jnp.float32)
            hb[:, cols] = jax.nn.gelu(pre, approximate=True).astype(jnp.bfloat16)
        for n in range(width // tile):
            cols = pl.ds(n * tile, tile)
            store(cols, jnp.dot(hb[...], second[:, cols], preferred_element_type=jnp.float32))

    def ffn(at):
        for way in (0, 1):
            slot_copy(way, at).wait_recv()

        def store(cols, result):
            result = result.astype(jnp.bfloat16)
            for way in (0, 1):
                lo = way * 2 * SLOTS
                rc[at, way, pl.ds(0, SLOTS), cols] = result[lo : lo + SLOTS]
                rs[at, way, :, cols] = result[lo + SLOTS : lo + 2 * SLOTS]

        two_dots(lambda: xb[at], win, wout, store)
        for way in (0, 1):
            result_copy(way, at).start()

    def shared_ffn():
        def store(cols, result):
            base[:, cols] = tok_ref[:, cols].astype(jnp.float32) + result

        two_dots(lambda: db[1, own], sin, sout, store)

    def dispatch(i, carry):
        step = i + 1

        for k in range(CHUNKS):
            block_copy(0, (0, i), i, k).wait_recv()

            @pl.when(step < far_r)
            def _():
                block_copy(0, (0, i), step, k).start()

            @pl.when(step <= far_l)
            def _():
                block_copy(1, (1, i), i, k).wait_recv()

            @pl.when(step < far_l)
            def _():
                block_copy(1, (1, i), step, k).start()

            if k == 0:
                meta_copy(0, (0, i), i).wait_recv()

                @pl.when(step < far_r)
                def _():
                    meta_copy(0, (0, i), step).start()

                @pl.when(step <= far_l)
                def _():
                    meta_copy(1, (1, i), i).wait_recv()

                @pl.when(step < far_l)
                def _():
                    meta_copy(1, (1, i), step).start()

                @pl.when(step == 1)
                def _():
                    gather(1, own)

                @pl.when(step > 1)
                def _():
                    gather(0, i - 1)

            if k == 1:

                @pl.when(step > 1)
                def _():
                    gather(1, i - 1)

            if k == 2:

                @pl.when(step >= FFN_FROM)
                def _():
                    ffn(i - 2)

            if k == 3:
                for hop in range(dp - 1):
                    for first, pair in ((0, (0, 1)), (2 * dp - 2, (2, 3))):

                        @pl.when(step == min(first + 2 * (hop + 1), far_r))
                        def _():
                            for a in pair:
                                weight_copy(a, hop).wait_recv()
                                if hop + 1 < dp - 1:
                                    weight_copy(a, hop + 1).start()
                                if hop == dp - 2:
                                    local_copy(a).wait()
                                    if a < 2:
                                        weight_copy(a + 2, 0).start()

        return carry

    lax.fori_loop(0, far_r, dispatch, 0)
    gather(0, far_r - 1)
    late = max(0, min(FFN_FROM - 3, far_r - 2))

    def last_units(i, carry):
        ffn(far_r - 2 + i)
        return carry

    lax.fori_loop(0, 2, last_units, 0)

    def combine(way, at, step, k, first):
        at_rows = piece(k)
        total = jnp.dot(st[way, at, at_rows, :], rc[at, way], preferred_element_type=jnp.float32)
        if not first:
            total = total + rb[way, step, at_rows, :].astype(jnp.float32)
        rb[way, step, at_rows, :] = total.astype(jnp.bfloat16)

    for way, far in ((1, far_l), (0, far_r)):
        result_copy(way, far - 1).wait_recv()
        for k in range(CHUNKS):
            combine(way, far - 1, 0, k, True)
        for k in range(CHUNKS):
            sum_copy(way, 0, k).start()

    def bring_back(r, carry):
        for k in range(CHUNKS):
            for way, far in ((0, far_r), (1, far_l)):

                @pl.when(r < far)
                def _():
                    if k == 0:
                        result_copy(way, far - 1 - r).wait_recv()
                    sum_copy(way, r - 1, k).wait_recv()
                    combine(way, far - 1 - r, r, k, False)
                    sum_copy(way, r, k).start()

            if k == 1:

                @pl.when(r <= late)
                def _():
                    ffn(late - r)

            if k == 2:

                @pl.when(r == min(8, far_r - 1))
                def _():
                    shared_ffn()

        return carry

    lax.fori_loop(1, far_r, bring_back, 0)

    result_copy(1, own).wait_recv()
    for k in range(CHUNKS):
        at_rows = piece(k)
        total = base[at_rows, :] + jnp.dot(
            st[1, own, at_rows, :], rc[own, 1], preferred_element_type=jnp.float32
        )
        for way, far in ((1, far_l), (0, far_r)):
            sum_copy(way, far - 1, k).wait_recv()
            total = total + rb[way, far, at_rows, :].astype(jnp.float32)
        out_ref[at_rows, :] = total.astype(jnp.bfloat16)

    def whole(ref, sem):
        return pltpu.make_async_copy(ref, ref, sem)

    for way, far in ((0, far_r), (1, far_l)):

        def drain(i, carry):
            whole(db.at[way, i], d_send.at[way, i]).wait()
            whole(mb.at[way, i], m_send.at[way, i]).wait()
            whole(rb.at[way, i], a_send.at[way, i]).wait()
            return carry

        lax.fori_loop(0, far, drain, 0)

        def drain_pair(i, carry):
            slot_copy(way, i).wait_send()
            result_copy(way, i).wait_send()
            return carry

        lax.fori_loop(0, far_r, drain_pair, 0)
    for a in range(4):
        for k in range(dp - 1):
            weight_copy(a, k).wait_send()


def per_device(mesh, tokens, expert_ids, gate_weights, expert_in, expert_out, shared_in, shared_out):
    rows, width = tokens.shape
    hidden = expert_in.shape[2]
    chips, dp = mesh.shape["expert"] // CORES, mesh.shape["dp"]
    far = chips // 2
    meta = jnp.concatenate([expert_ids.astype(jnp.float32).T, gate_weights.T], axis=0)
    vmem = pl.BlockSpec(memory_space=pltpu.VMEM)
    hbm = pl.BlockSpec(memory_space=pl.ANY)
    b16, f32, dma = jnp.bfloat16, jnp.float32, pltpu.SemaphoreType.DMA
    return pl.pallas_call(
        functools.partial(kernel, chips, dp),
        out_shape=jax.ShapeDtypeStruct((rows, width), b16),
        in_specs=[vmem, vmem, hbm, hbm, hbm, hbm],
        out_specs=vmem,
        scratch_shapes=[
            pltpu.VMEM((2, far, rows, width), b16),
            pltpu.VMEM((2, far, 16, rows), f32),
            pltpu.VMEM((2, far, rows, 2 * SLOTS), b16),
            pltpu.VMEM((far, 4 * SLOTS, width), b16),
            pltpu.VMEM((far, 2, SLOTS, width), b16),
            pltpu.VMEM((far, 2, 2 * SLOTS, width), b16),
            pltpu.VMEM((far, 2, SLOTS, width), b16),
            pltpu.VMEM((2, far + 1, rows, width), b16),
            pltpu.VMEM((rows, hidden), b16),
            pltpu.VMEM((rows, width), f32),
            pltpu.VMEM((width, hidden), b16),
            pltpu.VMEM((hidden, width), b16),
            pltpu.VMEM((width, hidden), b16),
            pltpu.VMEM((hidden, width), b16),
            dma((2, far, CHUNKS)),
            dma((2, far)),
            dma((2, far)),
            dma((2, far)),
            dma((2, far)),
            dma((2, far)),
            dma((2, far)),
            dma((2, far)),
            dma((2, far + 1, CHUNKS)),
            dma((2, far)),
            dma((4, dp - 1)),
            dma((4, dp - 1)),
            dma((4,)),
        ],
        compiler_params=pltpu.CompilerParams(
            collective_id=0, has_side_effects=True, vmem_limit_bytes=67043328
        ),
        name="moe_ring",
    )(tokens, meta, expert_in, expert_out, shared_in, shared_out)


def solution(mesh):
    placed = (
        P(("sweep", "expert", "dp"), None),
        P(("sweep", "expert", "dp"), None),
        P(("sweep", "expert", "dp"), None),
        P(("sweep", "expert"), "dp", None),
        P(("sweep", "expert"), None, "dp"),
        P(("sweep", "dp"), None),
        P("sweep", "dp"),
    )
    return jax.shard_map(
        functools.partial(per_device, mesh),
        mesh=mesh,
        in_specs=placed,
        out_specs=P(("sweep", "expert", "dp"), None),
        check_vma=False,
    )
```

```python
import functools

import jax
import jax.numpy as jnp
from jax import lax
from jax.experimental import pallas as pl
from jax.experimental.pallas import tpu as pltpu
from jax.sharding import PartitionSpec as P

CORES = 2
SLOTS = 32
PACK = 64
CHUNKS = 4
FFN_FROM = 8
STAGGER = 3
TILE = 256
MESH = pl.DeviceIdType.MESH


def kernel(
    chips, dp, tok_ref, meta_ref, win_ref, wout_ref, sin_ref, sout_ref, out_ref,
    nb, db, mb, st, sp, pq, pin, xb, rc, r16, rq, rp, rb, hb, base, win, wout, sin, sout,
    d_recv, d_send, m_recv, m_send, q_recv, q_send, f_recv, f_send,
    e_recv, e_send, g_recv, g_send, a_recv, a_send,
    w_recv, w_send, w_loc, p_recv, p_send, go,
):
    far = chips // 2
    full = far - 2
    pairs = far // 2
    rows, width = tok_ref.shape
    hidden = win.shape[2]
    part = rows // CHUNKS
    me = lax.axis_index("expert")
    core = lax.rem(me, CORES)
    chip = me // CORES
    right = lax.rem(chip + 1, chips) * CORES + core
    left = lax.rem(chip + chips - 1, chips) * CORES + core
    partner = chip * CORES + (1 - core)
    xi = lax.axis_index("dp")
    x_up, x_down = lax.rem(xi + 1, dp), lax.rem(xi + dp - 1, dp)
    towards = (right, left)

    barrier = pltpu.get_barrier_semaphore()
    for peer in ({"expert": right}, {"expert": left}, {"expert": partner}, {"dp": x_up}, {"dp": x_down}):
        pl.semaphore_signal(barrier, inc=1, device_id=peer, device_id_type=MESH)

    def remote(source, target, send, recv, device):
        return pltpu.make_async_remote_copy(
            src_ref=source, dst_ref=target, send_sem=send, recv_sem=recv,
            device_id=device, device_id_type=MESH,
        )

    def to(way):
        return {"expert": towards[way]}

    def piece(k):
        return pl.ds(k * part, part)

    def own_copy(way, k):
        return remote(nb.at[piece(k)], db.at[way, 0, piece(k)], d_send.at[way, 0], d_recv.at[way, 0, k], to(way))

    def block_copy(way, at, k):
        return remote(
            db.at[way, at, piece(k)], db.at[way, at + 1, piece(k)], d_send.at[way, at + 1], d_recv.at[way, at + 1, k], to(way)
        )

    def arrived(way, at, k):
        spot = db.at[way, at, piece(k)]
        return remote(spot, spot, d_send.at[way, at], d_recv.at[way, at, k], to(way))

    def meta_arrived(way, at):
        return remote(mb.at[way, at], mb.at[way, at], m_send.at[way, at], m_recv.at[way, at], to(way))

    def own_meta(way):
        return remote(meta_ref, mb.at[way, 0], m_send.at[way, 0], m_recv.at[way, 0], to(way))

    def meta_copy(way, at):
        return remote(mb.at[way, at], mb.at[way, at + 1], m_send.at[way, at + 1], m_recv.at[way, at + 1], to(way))

    def pack_copy(way, half):
        lanes = pl.ds(half * PACK // 2, PACK // 2)
        return remote(pq.at[way, lanes], pin.at[way, lanes], q_send.at[way, half], q_recv.at[way, half], to(way))

    def last_copy(way):
        return remote(
            pin.at[way, pl.ds(PACK // 2, PACK // 2)],
            xb.at[way, pairs - 1, pl.ds(2 * SLOTS + way * SLOTS, SLOTS)],
            f_send.at[way], f_recv.at[way], to(way),
        )

    def last_back(way):
        return remote(rc.at[far - 1, way, pl.ds(way * SLOTS, SLOTS)], r16.at[way], e_send.at[way], e_recv.at[way], to(1 - way))

    def pack_back(way, half):
        lanes = pl.ds(half * PACK // 2, PACK // 2)
        return remote(rq.at[way, lanes], rp.at[way, lanes], g_send.at[way, half], g_recv.at[way, half], to(1 - way))

    def sum_copy(way, step, k):
        return remote(
            rb.at[way, step, piece(k)], rb.at[way, step + 1, piece(k)], a_send.at[way, step], a_recv.at[way, step + 1, k],
            to(1 - way),
        )

    d_part, f_part = win_ref.shape[1], wout_ref.shape[2]
    shards = (win_ref.at[0], wout_ref.at[0], sin_ref, sout_ref)

    def region(a, shard):
        if a % 2 == 0:
            where = pl.ds(shard * d_part, d_part)
            return win.at[core, where, :] if a == 0 else sin.at[where, :]
        where = pl.ds(pl.multiple_of(shard * f_part, 128), f_part)
        return wout.at[core, :, where] if a == 1 else sout.at[:, where]

    def shard_at(a, k):
        return lax.rem(xi + dp - k, dp) if a % 2 == 0 else lax.rem(xi + k, dp)

    def weight_copy(a, k):
        spot = region(a, shard_at(a, k))
        return remote(
            shards[a] if k == 0 else spot, spot, w_send.at[a, k], w_recv.at[a, k], {"dp": x_up if a % 2 == 0 else x_down}
        )

    def twin_copy(a, k):
        spot = region(a, shard_at(a, k))
        return remote(shards[a] if k == 0 else spot, spot, p_send.at[a, k], p_recv.at[a, k], {"expert": partner})

    def twin_wait(a, k):
        shard = shard_at(a, k)
        if a == 0:
            spot = win.at[1 - core, pl.ds(shard * d_part, d_part), :]
        else:
            spot = wout.at[1 - core, :, pl.ds(pl.multiple_of(shard * f_part, 128), f_part)]
        return remote(spot, spot, p_send.at[a, k], p_recv.at[a, k], {"expert": partner})

    def local_copy(a):
        return pltpu.make_async_copy(shards[a], region(a, xi), w_loc.at[a])

    def norm(k):
        for half in range(part // 16):
            at_rows = pl.ds(k * part + half * 16, 16)
            values = tok_ref[at_rows, :].astype(jnp.float32)
            center = values - jnp.mean(values, axis=-1, keepdims=True)
            spread = jnp.mean(center * center, axis=-1, keepdims=True)
            nb[at_rows, :] = (center * lax.rsqrt(spread + 1e-06)).astype(jnp.bfloat16)

    norm(0)
    norm(1)
    pl.semaphore_wait(barrier, 5)
    for a in (0, 1):
        weight_copy(a, 0).start()

    @pl.when(core > 0)
    def _():
        pl.semaphore_wait(go, 1)

    for way in (0, 1):
        own_meta(way).start()
    for k in range(CHUNKS):
        for way in (0, 1):
            own_copy(way, k).start()
        if k + 2 < CHUNKS:
            norm(k + 2)
    for a in range(4):
        local_copy(a).start()
    for a in (0, 1):
        twin_copy(a, 0).start()

    def places(meta, experts):
        meta = meta.astype(jnp.float32)
        ids, gates = meta[0:8], meta[8:16]
        match, gate = [], []
        for expert in experts:
            hit = ids == expert.astype(jnp.float32)
            match.append(jnp.sum(jnp.where(hit, 1.0, 0.0), axis=0, keepdims=True))
            gate.append(jnp.sum(jnp.where(hit, gates, 0.0), axis=0, keepdims=True))
        both = jnp.concatenate([jnp.broadcast_to(m, (8, rows)) for m in match], axis=0)
        before = lax.broadcasted_iota(jnp.int32, (rows, rows), 0) < lax.broadcasted_iota(jnp.int32, (rows, rows), 1)
        earlier = jnp.dot(
            both.astype(jnp.bfloat16),
            jnp.where(before, 1.0, 0.0).astype(jnp.bfloat16),
            preferred_element_type=jnp.float32,
        )
        slot = jnp.where(both > 0.5, earlier, -1.0)
        return [slot[8 * i : 8 * i + 8] for i in range(len(experts))], gate

    def row_of(count):
        return lax.broadcasted_iota(jnp.int32, (count, rows), 0).astype(jnp.float32)

    def choose(meta):
        slot, gate = places(meta, (chip * CORES, chip * CORES + 1))
        pick, spread = [], []
        for i in (0, 1):
            here = jnp.concatenate([slot[i]] * (SLOTS // 8), axis=0) == row_of(SLOTS)
            pick.append(jnp.where(here, 1.0, 0.0))
            spread.append(jnp.where(here, jnp.broadcast_to(gate[i], (SLOTS, rows)), 0.0))
        return jnp.concatenate(pick, axis=0).astype(jnp.bfloat16), jnp.concatenate(spread, axis=0).T.astype(jnp.bfloat16)

    def unit_rows(at, way):
        return pl.ds(pl.multiple_of(lax.rem(at, 2) * 2 * SLOTS + way * SLOTS, SLOTS), SLOTS)

    def gather(way, at):
        picked, st[way, at] = choose(mb[way, at])
        for n in range(width // TILE):
            cols = pl.ds(n * TILE, TILE)
            got = jnp.dot(picked, db[way, at, :, cols], preferred_element_type=jnp.float32).astype(jnp.bfloat16)
            for e in (0, 1):
                xb[e, at // 2, unit_rows(at, way), cols] = got[e * SLOTS : e * SLOTS + SLOTS]

    def gather_own():
        picked, spread = choose(meta_ref[...])
        sp[2] = spread
        for n in range(width // TILE):
            cols = pl.ds(n * TILE, TILE)
            got = jnp.dot(picked, nb[:, cols], preferred_element_type=jnp.float32).astype(jnp.bfloat16)
            for e in (0, 1):
                xb[e, pairs - 1, pl.ds(2 * SLOTS + (1 - e) * SLOTS, SLOTS), cols] = got[e * SLOTS : e * SLOTS + SLOTS]

    def pack(way):
        ahead = 1 - 2 * way
        near = lax.rem(chip + chips + ahead, chips) * CORES
        last = lax.rem(chip + chips + 2 * ahead, chips) * CORES + way
        meta = mb[way, full - 1]
        slot, gate = places(meta, (near, near + 1))
        slot_last, gate_last = places(meta, (last, last))
        slot, gate = slot + slot_last[:1], gate + gate_last[:1]
        slot = [jnp.concatenate([s, s], axis=0) for s in slot]
        row = row_of(16)
        pick, spread = [], []
        for s, g in zip(slot, gate):
            pick.append(jnp.where(s == row, 1.0, 0.0))
            spread.append(jnp.where(s == row, jnp.broadcast_to(g, (16, rows)), 0.0))
        tail_pick, tail_spread = jnp.zeros((16, rows), jnp.float32), jnp.zeros((16, rows), jnp.float32)
        for i, (s, g) in enumerate(zip(slot, gate)):
            inside = jnp.where((row >= 4 * i) & (row < 4 * i + 4), row + (16 - 4 * i), -2.0)
            tail_pick = jnp.where(s == inside, 1.0, tail_pick)
            tail_spread = jnp.where(s == inside, jnp.broadcast_to(g, (16, rows)), tail_spread)
        picked = jnp.concatenate(pick + [tail_pick], axis=0).astype(jnp.bfloat16)
        sp[way] = jnp.concatenate(spread + [tail_spread], axis=0).T.astype(jnp.bfloat16)
        for n in range(width // TILE):
            cols = pl.ds(n * TILE, TILE)
            pq[way, :, cols] = jnp.dot(
                picked, db[way, full - 1, :, cols], preferred_element_type=jnp.float32
            ).astype(jnp.bfloat16)

    def two_dots(source, first, second, store):
        for n in range(hidden // TILE):
            cols = pl.ds(n * TILE, TILE)
            pre = jnp.dot(source(), first(cols), preferred_element_type=jnp.float32)
            hb[:, cols] = jax.nn.gelu(pre, approximate=True).astype(jnp.bfloat16)
        for n in range(width // TILE):
            cols = pl.ds(n * TILE, TILE)
            store(cols, jnp.dot(hb[...], second(cols), preferred_element_type=jnp.float32))

    def ffn(call):
        pair, e = call // 2, lax.rem(call, 2)

        def store(cols, result):
            result = result.astype(jnp.bfloat16)
            for h in (0, 1):
                for way in (0, 1):
                    lo = (2 * h + way) * SLOTS
                    rc[2 * pair + h, way, pl.ds(pl.multiple_of(e * SLOTS, SLOTS), SLOTS), cols] = result[lo : lo + SLOTS]

        two_dots(lambda: xb[e, pair], lambda cols: win[e, :, cols], lambda cols: wout[e, :, cols], store)

    def shared_ffn():
        def store(cols, result):
            base[:, cols] = tok_ref[:, cols].astype(jnp.float32) + result

        two_dots(lambda: nb[...], lambda cols: sin[:, cols], lambda cols: sout[:, cols], store)

    def calls_by(step_index):
        done = jnp.minimum(2 * (step_index // 2), 2 * (step_index + 1 - FFN_FROM))
        return jnp.maximum(done, 0)

    def dispatch(i, carry):
        lo, hi = calls_by(i - 1), calls_by(i)
        lo = jnp.where(i == 0, 0, lo)
        for k in range(CHUNKS):
            for way in (0, 1):
                arrived(way, i, k).wait_recv()

                @pl.when(i + 1 < full)
                def _():
                    block_copy(way, i, k).start()

                if k == 0:
                    meta_arrived(way, i).wait_recv()

                    @pl.when(i + 1 < full)
                    def _():
                        meta_copy(way, i).start()

            if k == 0:

                @pl.when(i == 0)
                def _():
                    gather_own()

                @pl.when(i > 0)
                def _():
                    gather(0, i - 1)

            if k == 1:

                @pl.when(i > 0)
                def _():
                    gather(1, i - 1)

            if k >= 2:

                @pl.when(lo + (k - 2) < hi)
                def _():
                    ffn(lo + (k - 2))

            if k == 3:

                @pl.when((i == min(STAGGER, full) - 1) & (core == 0))
                def _():
                    pl.semaphore_signal(go, inc=1, device_id={"expert": partner}, device_id_type=MESH)

                for hop in range(dp - 1):
                    for first, pair in ((0, (0, 1)), (2 * dp - 2, (2, 3))):

                        @pl.when(i == min(first + 2 * hop + 1, full - 1))
                        def _():
                            for a in pair:
                                weight_copy(a, hop).wait_recv()
                                if hop + 1 < dp - 1:
                                    weight_copy(a, hop + 1).start()
                                if a < 2:
                                    twin_copy(a, hop + 1).start()
                                if hop == dp - 2:
                                    local_copy(a).wait()
                                    if a < 2:
                                        weight_copy(a + 2, 0).start()
                                        for j in range(dp):
                                            twin_wait(a, j).wait_recv()

        return carry

    lax.fori_loop(0, full, dispatch, 0)
    for way in (0, 1):
        pack(way)
        for half in (1, 0):
            pack_copy(way, half).start()
    for way in (0, 1):
        gather(way, full - 1)
    started = max(0, min(2 * ((full - 1) // 2), 2 * (full - FFN_FROM)))
    rest = list(range(started, 2 * (pairs - 1)))

    def run(calls):
        if calls:

            def body(c, carry):
                ffn(c)
                return carry

            lax.fori_loop(calls[0], calls[-1] + 1, body, 0)

    run(rest[: len(rest) // 2])
    for way in (0, 1):
        pack_copy(way, 1).wait_recv()
        last_copy(way).start()
    for way in (0, 1):
        pack_copy(way, 0).wait_recv()
        for e in (0, 1):
            xb[e, pairs - 1, pl.ds(way * SLOTS, 16), :] = pin[way, pl.ds(e * 16, 16), :]
            xb[e, pairs - 1, pl.ds(way * SLOTS + 16, 16), :] = pin[way, pl.ds(48, 16), :]
    run(rest[len(rest) // 2 :])

    def last_unit(e, carry):
        for way in (0, 1):

            @pl.when(e == way)
            def _():
                last_copy(way).wait_recv()

        ffn(2 * (pairs - 1) + e)
        for way in (0, 1):

            @pl.when(e == way)
            def _():
                last_back(way).start()

        return carry

    lax.fori_loop(0, 2, last_unit, 0)
    tail = lax.broadcasted_iota(jnp.int32, (16, width), 0)
    for way in (0, 1):
        for e in (0, 1):
            rq[way, pl.ds(e * 16, 16), :] = rc[far - 2, way, pl.ds(e * SLOTS, 16), :]
    for way in (0, 1):
        pack_back(way, 0).start()
    for way in (0, 1):
        last_back(way).wait_recv()
        rq[way, pl.ds(32, 16), :] = r16[way, pl.ds(0, 16), :]
        tails = [rc[far - 2, way, pl.ds(e * SLOTS + 16, 16), :].astype(jnp.float32) for e in (0, 1)]
        tails.append(r16[way, pl.ds(16, 16), :].astype(jnp.float32))
        rq[way, pl.ds(48, 16), :] = jnp.where(
            tail < 4, tails[0], jnp.where(tail < 8, tails[1], tails[2])
        ).astype(jnp.bfloat16)
    for way in (0, 1):
        pack_back(way, 1).start()

    def combine(way, at, step, k, first):
        at_rows = piece(k)
        total = jnp.dot(st[way, at, at_rows, :], rc[at, way], preferred_element_type=jnp.float32)
        if first:
            total = total + jnp.dot(sp[way, at_rows, :], rp[way], preferred_element_type=jnp.float32)
        else:
            total = total + rb[way, step, at_rows, :].astype(jnp.float32)
        rb[way, step, at_rows, :] = total.astype(jnp.bfloat16)

    for way in (0, 1):
        for half in (0, 1):
            pack_back(way, half).wait_recv()
    for k in range(CHUNKS):
        for way in (0, 1):
            combine(way, full - 1, 0, k, True)
        for way in (0, 1):
            sum_copy(way, 0, k).start()

    def bring_back(j, carry):
        for k in range(CHUNKS):
            for way in (0, 1):
                sum_copy(way, j - 1, k).wait_recv()
                combine(way, full - 1 - j, j, k, False)
            for way in (0, 1):
                sum_copy(way, j, k).start()
            if k == 2:

                @pl.when(j == min(6, full - 1))
                def _():
                    shared_ffn()

        return carry

    lax.fori_loop(1, full, bring_back, 0)

    for k in range(CHUNKS):
        at_rows = piece(k)
        total = base[at_rows, :]
        for e in (0, 1):
            total = total + jnp.dot(
                sp[2, at_rows, e * SLOTS : (e + 1) * SLOTS],
                rc[far - 1, 1 - e, pl.ds(e * SLOTS, SLOTS), :],
                preferred_element_type=jnp.float32,
            )
        for way in (0, 1):
            sum_copy(way, full - 1, k).wait_recv()
            total = total + rb[way, full, at_rows, :].astype(jnp.float32)
        out_ref[at_rows, :] = total.astype(jnp.bfloat16)

    def whole(ref, sem):
        return pltpu.make_async_copy(ref, ref, sem)

    for way in (0, 1):

        def drain(i, carry):
            whole(db.at[way, i], d_send.at[way, i]).wait()
            whole(mb.at[way, i], m_send.at[way, i]).wait()
            whole(rb.at[way, i], a_send.at[way, i]).wait()
            return carry

        lax.fori_loop(0, full, drain, 0)
        for half in (0, 1):
            pack_copy(way, half).wait_send()
            pack_back(way, half).wait_send()
        last_copy(way).wait_send()
        last_back(way).wait_send()
    for a in range(4):
        for k in range(dp - 1):
            weight_copy(a, k).wait_send()
        if a < 2:
            for k in range(dp):
                twin_copy(a, k).wait_send()


def per_device(mesh, tokens, expert_ids, gate_weights, expert_in, expert_out, shared_in, shared_out):
    rows, width = tokens.shape
    hidden = expert_in.shape[2]
    chips, dp = mesh.shape["expert"] // CORES, mesh.shape["dp"]
    far = chips // 2
    full = far - 2
    meta = jnp.concatenate([expert_ids.astype(jnp.bfloat16).T, gate_weights.astype(jnp.bfloat16).T], axis=0)
    vmem = pl.BlockSpec(memory_space=pltpu.VMEM)
    hbm = pl.BlockSpec(memory_space=pl.ANY)
    b16, f32, dma = jnp.bfloat16, jnp.float32, pltpu.SemaphoreType.DMA
    return pl.pallas_call(
        functools.partial(kernel, chips, dp),
        out_shape=jax.ShapeDtypeStruct((rows, width), b16),
        in_specs=[vmem, vmem, hbm, hbm, hbm, hbm],
        out_specs=vmem,
        scratch_shapes=[
            pltpu.VMEM((rows, width), b16),
            pltpu.VMEM((2, full, rows, width), b16),
            pltpu.VMEM((2, full, 16, rows), b16),
            pltpu.VMEM((2, full, rows, 2 * SLOTS), b16),
            pltpu.VMEM((3, rows, PACK), b16),
            pltpu.VMEM((2, PACK, width), b16),
            pltpu.VMEM((2, PACK, width), b16),
            pltpu.VMEM((2, far // 2, 4 * SLOTS, width), b16),
            pltpu.VMEM((far, 2, 2 * SLOTS, width), b16),
            pltpu.VMEM((2, SLOTS, width), b16),
            pltpu.VMEM((2, PACK, width), b16),
            pltpu.VMEM((2, PACK, width), b16),
            pltpu.VMEM((2, full + 1, rows, width), b16),
            pltpu.VMEM((rows, hidden), b16),
            pltpu.VMEM((rows, width), f32),
            pltpu.VMEM((2, width, hidden), b16),
            pltpu.VMEM((2, hidden, width), b16),
            pltpu.VMEM((width, hidden), b16),
            pltpu.VMEM((hidden, width), b16),
            dma((2, full, CHUNKS)),
            dma((2, full)),
            dma((2, full)),
            dma((2, full)),
            dma((2, 2)),
            dma((2, 2)),
            dma((2,)),
            dma((2,)),
            dma((2,)),
            dma((2,)),
            dma((2, 2)),
            dma((2, 2)),
            dma((2, full + 1, CHUNKS)),
            dma((2, full)),
            dma((4, dp - 1)),
            dma((4, dp - 1)),
            dma((4,)),
            dma((2, dp)),
            dma((2, dp)),
            pltpu.SemaphoreType.REGULAR,
        ],
        compiler_params=pltpu.CompilerParams(
            collective_id=0, has_side_effects=True, vmem_limit_bytes=67043328
        ),
        name="moe_ring",
    )(tokens, meta, expert_in, expert_out, shared_in, shared_out)


def solution(mesh):
    placed = (
        P(("sweep", "expert", "dp"), None),
        P(("sweep", "expert", "dp"), None),
        P(("sweep", "expert", "dp"), None),
        P(("sweep", "expert"), "dp", None),
        P(("sweep", "expert"), None, "dp"),
        P(("sweep", "dp"), None),
        P("sweep", "dp"),
    )
    return jax.shard_map(
        functools.partial(per_device, mesh),
        mesh=mesh,
        in_specs=placed,
        out_specs=P(("sweep", "expert", "dp"), None),
        check_vma=False,
    )
```

```python
import functools

import jax
import jax.numpy as jnp
from jax import lax
from jax.experimental import pallas as pl
from jax.experimental.pallas import tpu as pltpu
from jax.sharding import PartitionSpec as P

CORES = 2
SLOTS = 32
NEAR = 48
CHUNKS = 4
FFN_FROM = 8
TILE = 256
MESH = pl.DeviceIdType.MESH


def kernel(
    chips, dp, tok_ref, ids_ref, gates_ref, win_ref, wout_ref, sin_ref, sout_ref, out_ref,
    mo, nb, db, mb, st, sp, so, pq, pin, xb, rc, rq, rp, rb, hb, base, win, wout, sin, sout,
    d_recv, d_send, m_recv, m_send, q_recv, q_send, f_recv, f_send,
    e_recv, e_send, g_recv, g_send, a_recv, a_send,
    w_recv, w_send, w_loc, p_recv, p_send,
):
    far = chips // 2
    full = far - 2
    pairs = far // 2
    rows, width = tok_ref.shape
    hidden = win.shape[2]
    part = rows // CHUNKS
    me = lax.axis_index("expert")
    core = lax.rem(me, CORES)
    chip = me // CORES
    right = lax.rem(chip + 1, chips) * CORES + core
    left = lax.rem(chip + chips - 1, chips) * CORES + core
    partner = chip * CORES + (1 - core)
    xi = lax.axis_index("dp")
    x_up, x_down = lax.rem(xi + 1, dp), lax.rem(xi + dp - 1, dp)
    towards = (right, left)
    right2 = lax.rem(chip + 2, chips) * CORES + core
    left2 = lax.rem(chip + chips - 2, chips) * CORES + core

    barrier = pltpu.get_barrier_semaphore()
    peers = [{"expert": p} for p in (right, left, partner, right2, left2)] + [{"dp": x_up}, {"dp": x_down}]
    for peer in peers:
        pl.semaphore_signal(barrier, inc=1, device_id=peer, device_id_type=MESH)

    def remote(source, target, send, recv, device):
        return pltpu.make_async_remote_copy(
            src_ref=source, dst_ref=target, send_sem=send, recv_sem=recv,
            device_id=device, device_id_type=MESH,
        )

    def to(way):
        return {"expert": towards[way]}

    def piece(k):
        return pl.ds(k * part, part)

    def own_copy(way, k):
        return remote(nb.at[piece(k)], db.at[way, 0, piece(k)], d_send.at[way, 0], d_recv.at[way, 0, k], to(way))

    def block_copy(way, at, k):
        return remote(
            db.at[way, at, piece(k)], db.at[way, at + 1, piece(k)], d_send.at[way, at + 1], d_recv.at[way, at + 1, k], to(way)
        )

    def arrived(way, at, k):
        spot = db.at[way, at, piece(k)]
        return remote(spot, spot, d_send.at[way, at], d_recv.at[way, at, k], to(way))

    def meta_arrived(way, at):
        return remote(mb.at[way, at], mb.at[way, at], m_send.at[way, at], m_recv.at[way, at], to(way))

    def own_meta(way):
        return remote(mo, mb.at[way, 0], m_send.at[way, 0], m_recv.at[way, 0], to(way))

    def meta_copy(way, at):
        return remote(mb.at[way, at], mb.at[way, at + 1], m_send.at[way, at + 1], m_recv.at[way, at + 1], to(way))

    def near_copy(way):
        return remote(pq.at[way, pl.ds(0, NEAR)], pin.at[way], q_send.at[way], q_recv.at[way], to(way))

    def last_copy(way):
        return remote(
            pq.at[way, pl.ds(NEAR, SLOTS)],
            xb.at[way, pairs - 1, pl.ds(pl.multiple_of(2 * SLOTS + way * SLOTS, SLOTS), SLOTS)],
            f_send.at[way], f_recv.at[way], {"expert": jnp.where(way == 0, right2, left2)},
        )

    def last_back(way):
        return remote(
            rc.at[far - 1, way, pl.ds(pl.multiple_of(way * SLOTS, SLOTS), SLOTS)],
            rp.at[way, pl.ds(NEAR, SLOTS)],
            e_send.at[way], e_recv.at[way], {"expert": jnp.where(way == 0, left2, right2)},
        )

    def near_back(way):
        return remote(rq.at[way], rp.at[way, pl.ds(0, NEAR)], g_send.at[way], g_recv.at[way], to(1 - way))

    def sum_copy(way, step, k):
        return remote(
            rb.at[way, step, piece(k)], rb.at[way, step + 1, piece(k)], a_send.at[way, step], a_recv.at[way, step + 1, k],
            to(1 - way),
        )

    d_part, f_part = win_ref.shape[1], wout_ref.shape[2]
    shards = (win_ref.at[0], wout_ref.at[0], sin_ref, sout_ref)

    def region(a, shard):
        if a % 2 == 0:
            where = pl.ds(shard * d_part, d_part)
            return win.at[core, where, :] if a == 0 else sin.at[where, :]
        where = pl.ds(pl.multiple_of(shard * f_part, 128), f_part)
        return wout.at[core, :, where] if a == 1 else sout.at[:, where]

    def shard_at(a, k):
        return lax.rem(xi + dp - k, dp) if a % 2 == 0 else lax.rem(xi + k, dp)

    def weight_copy(a, k):
        spot = region(a, shard_at(a, k))
        return remote(
            shards[a] if k == 0 else spot, spot, w_send.at[a, k], w_recv.at[a, k], {"dp": x_up if a % 2 == 0 else x_down}
        )

    def twin_copy(a, k):
        spot = region(a, shard_at(a, k))
        return remote(shards[a] if k == 0 else spot, spot, p_send.at[a, k], p_recv.at[a, k], {"expert": partner})

    def twin_wait(a, k):
        shard = shard_at(a, k)
        if a == 0:
            spot = win.at[1 - core, pl.ds(shard * d_part, d_part), :]
        else:
            spot = wout.at[1 - core, :, pl.ds(pl.multiple_of(shard * f_part, 128), f_part)]
        return remote(spot, spot, p_send.at[a, k], p_recv.at[a, k], {"expert": partner})

    def local_copy(a):
        return pltpu.make_async_copy(shards[a], region(a, xi), w_loc.at[a])

    def norm(k):
        for half in range(part // 16):
            at_rows = pl.ds(k * part + half * 16, 16)
            values = tok_ref[at_rows, :].astype(jnp.float32)
            center = values - jnp.mean(values, axis=-1, keepdims=True)
            spread = jnp.mean(center * center, axis=-1, keepdims=True)
            nb[at_rows, :] = (center * lax.rsqrt(spread + 1e-06)).astype(jnp.bfloat16)

    mo[...] = jnp.concatenate([ids_ref[...].astype(jnp.float32), gates_ref[...]], axis=0).astype(jnp.bfloat16)
    norm(0)
    norm(1)
    pl.semaphore_wait(barrier, len(peers))
    for a in (0, 1):
        weight_copy(a, 0).start()

    for way in (0, 1):
        own_meta(way).start()
    for k in range(CHUNKS):
        for way in (0, 1):
            own_copy(way, k).start()
        if k + 2 < CHUNKS:
            norm(k + 2)
    for a in range(4):
        local_copy(a).start()
    for a in (0, 1):
        twin_copy(a, 0).start()

    def places(meta, experts):
        meta = meta.astype(jnp.float32)
        ids, gates = meta[0:8], meta[8:16]
        match, gate = [], []
        for expert in experts:
            hit = ids == expert.astype(jnp.float32)
            match.append(jnp.sum(jnp.where(hit, 1.0, 0.0), axis=0, keepdims=True))
            gate.append(jnp.sum(jnp.where(hit, gates, 0.0), axis=0, keepdims=True))
        both = jnp.concatenate([jnp.broadcast_to(m, (8, rows)) for m in match], axis=0)
        before = lax.broadcasted_iota(jnp.int32, (rows, rows), 0) < lax.broadcasted_iota(jnp.int32, (rows, rows), 1)
        earlier = jnp.dot(
            both.astype(jnp.bfloat16),
            jnp.where(before, 1.0, 0.0).astype(jnp.bfloat16),
            preferred_element_type=jnp.float32,
        )
        slot = jnp.where(both > 0.5, earlier, -1.0)
        return [slot[8 * i : 8 * i + 8] for i in range(len(experts))], gate

    def row_of(count):
        return lax.broadcasted_iota(jnp.int32, (count, rows), 0).astype(jnp.float32)

    def choose(meta):
        slot, gate = places(meta, (chip * CORES, chip * CORES + 1))
        pick, spread = [], []
        for i in (0, 1):
            here = jnp.concatenate([slot[i]] * (SLOTS // 8), axis=0) == row_of(SLOTS)
            pick.append(jnp.where(here, 1.0, 0.0))
            spread.append(jnp.where(here, jnp.broadcast_to(gate[i], (SLOTS, rows)), 0.0))
        return jnp.concatenate(pick, axis=0).astype(jnp.bfloat16), jnp.concatenate(spread, axis=0).T.astype(jnp.bfloat16)

    def unit_rows(at, way):
        return pl.ds(pl.multiple_of(lax.rem(at, 2) * 2 * SLOTS + way * SLOTS, SLOTS), SLOTS)

    def gather(way, at):
        picked, st[way, at] = choose(mb[way, at])
        for n in range(width // TILE):
            cols = pl.ds(n * TILE, TILE)
            got = jnp.dot(picked, db[way, at, :, cols], preferred_element_type=jnp.float32).astype(jnp.bfloat16)
            for e in (0, 1):
                xb[e, at // 2, unit_rows(at, way), cols] = got[e * SLOTS : e * SLOTS + SLOTS]

    def gather_own():
        picked, spread = choose(mo[...])
        so[...] = spread
        for n in range(width // TILE):
            cols = pl.ds(n * TILE, TILE)
            got = jnp.dot(picked, nb[:, cols], preferred_element_type=jnp.float32).astype(jnp.bfloat16)
            for e in (0, 1):
                xb[e, pairs - 1, pl.ds(2 * SLOTS + (1 - e) * SLOTS, SLOTS), cols] = got[e * SLOTS : e * SLOTS + SLOTS]

    def pack(way):
        ahead = 1 - 2 * way
        near = lax.rem(chip + chips + ahead, chips) * CORES
        last = lax.rem(chip + chips + 2 * ahead, chips) * CORES + way
        meta = mb[way, full - 1]
        slot, gate = places(meta, (near, near + 1))
        slot_last, gate_last = places(meta, (last, last))
        row = row_of(16)
        pick, spread = [], []
        tail_pick, tail_spread = jnp.zeros((16, rows), jnp.float32), jnp.zeros((16, rows), jnp.float32)
        for i in (0, 1):
            where = jnp.concatenate([slot[i], slot[i]], axis=0)
            weight = jnp.broadcast_to(gate[i], (16, rows))
            pick.append(jnp.where(where == row, 1.0, 0.0))
            spread.append(jnp.where(where == row, weight, 0.0))
            inside = jnp.where((row >= 4 * i) & (row < 4 * i + 4), row + (16 - 4 * i), -2.0)
            tail_pick = jnp.where(where == inside, 1.0, tail_pick)
            tail_spread = jnp.where(where == inside, weight, tail_spread)
        here = jnp.concatenate([slot_last[0]] * (SLOTS // 8), axis=0) == row_of(SLOTS)
        pick += [tail_pick, jnp.where(here, 1.0, 0.0)]
        spread += [tail_spread, jnp.where(here, jnp.broadcast_to(gate_last[0], (SLOTS, rows)), 0.0)]
        picked = jnp.concatenate(pick, axis=0).astype(jnp.bfloat16)
        filler = [jnp.zeros((rows - NEAR - SLOTS, rows), jnp.float32)]
        sp[way] = jnp.concatenate(spread + filler, axis=0).T[:, : NEAR + SLOTS].astype(jnp.bfloat16)
        for n in range(width // TILE):
            cols = pl.ds(n * TILE, TILE)
            pq[way, :, cols] = jnp.dot(
                picked, db[way, full - 1, :, cols], preferred_element_type=jnp.float32
            ).astype(jnp.bfloat16)

    def two_dots(count, source, first, second, store):
        for n in range(hidden // TILE):
            cols = pl.ds(n * TILE, TILE)
            pre = jnp.dot(source(), first(cols), preferred_element_type=jnp.float32)
            hb[:count, cols] = jax.nn.gelu(pre, approximate=True).astype(jnp.bfloat16)
        for n in range(width // TILE):
            cols = pl.ds(n * TILE, TILE)
            store(cols, jnp.dot(hb[:count], second(cols), preferred_element_type=jnp.float32))

    def ffn(call):
        pair, e = call // 2, lax.rem(call, 2)

        def store(cols, result):
            result = result.astype(jnp.bfloat16)
            for h in (0, 1):
                for way in (0, 1):
                    lo = (2 * h + way) * SLOTS
                    rc[2 * pair + h, way, pl.ds(pl.multiple_of(e * SLOTS, SLOTS), SLOTS), cols] = result[lo : lo + SLOTS]

        two_dots(4 * SLOTS, lambda: xb[e, pair], lambda cols: win[e, :, cols], lambda cols: wout[e, :, cols], store)

    def ffn_one(h, e):
        def store(cols, result):
            result = result.astype(jnp.bfloat16)
            for way in (0, 1):
                rc[far - 2 + h, way, pl.ds(pl.multiple_of(e * SLOTS, SLOTS), SLOTS), cols] = result[
                    way * SLOTS : (way + 1) * SLOTS
                ]

        source = pl.ds(2 * SLOTS * h, 2 * SLOTS)
        two_dots(
            2 * SLOTS, lambda: xb[e, pairs - 1, source, :], lambda cols: win[e, :, cols], lambda cols: wout[e, :, cols], store
        )

    def shared_ffn():
        def store(cols, result):
            base[:, cols] = tok_ref[:, cols].astype(jnp.float32) + result

        two_dots(rows, lambda: nb[...], lambda cols: sin[:, cols], lambda cols: sout[:, cols], store)

    def calls_by(step_index):
        done = jnp.minimum(2 * (step_index // 2), 2 * (step_index + 1 - FFN_FROM))
        return jnp.maximum(done, 0)

    def dispatch(i, carry):
        lo, hi = calls_by(i - 1), calls_by(i)
        lo = jnp.where(i == 0, 0, lo)
        for k in range(CHUNKS):
            for way in (0, 1):
                arrived(way, i, k).wait_recv()

                @pl.when(i + 1 < full)
                def _():
                    block_copy(way, i, k).start()

                if k == 0:
                    meta_arrived(way, i).wait_recv()

                    @pl.when(i + 1 < full)
                    def _():
                        meta_copy(way, i).start()

            if k == 0:

                @pl.when(i == 0)
                def _():
                    gather_own()

                @pl.when(i > 0)
                def _():
                    gather(0, i - 1)

            if k == 1:

                @pl.when(i > 0)
                def _():
                    gather(1, i - 1)

            if k >= 2:

                @pl.when(lo + (k - 2) < hi)
                def _():
                    ffn(lo + (k - 2))

            if k == 3:

                for hop in range(dp - 1):
                    for first, pair in ((0, (0, 1)), (2 * dp - 2, (2, 3))):

                        @pl.when(i == min(first + 2 * hop + 1, full - 1))
                        def _():
                            for a in pair:
                                weight_copy(a, hop).wait_recv()
                                if hop + 1 < dp - 1:
                                    weight_copy(a, hop + 1).start()
                                if a < 2:
                                    twin_copy(a, hop + 1).start()
                                if hop == dp - 2:
                                    local_copy(a).wait()
                                    if a < 2:
                                        weight_copy(a + 2, 0).start()
                                        for j in range(dp):
                                            twin_wait(a, j).wait_recv()

        return carry

    lax.fori_loop(0, full, dispatch, 0)
    for way in (0, 1):
        pack(way)
    for way in (0, 1):
        last_copy(way).start()
        near_copy(way).start()
    for way in (0, 1):
        gather(way, full - 1)
    started = max(0, min(2 * ((full - 1) // 2), 2 * (full - FFN_FROM)))
    rest = list(range(started, 2 * (pairs - 1)))

    def run(calls):
        if calls:

            def body(c, carry):
                ffn(c)
                return carry

            lax.fori_loop(calls[0], calls[-1] + 1, body, 0)

    run(rest[: len(rest) // 2])

    def last_unit(e, carry):
        last_copy(e).wait_recv()
        ffn_one(1, e)
        last_back(e).start()
        return carry

    lax.fori_loop(0, 2, last_unit, 0)
    for way in (0, 1):
        near_copy(way).wait_recv()
        for e in (0, 1):
            xb[e, pairs - 1, pl.ds(way * SLOTS, 16), :] = pin[way, pl.ds(e * 16, 16), :]
            xb[e, pairs - 1, pl.ds(way * SLOTS + 16, 16), :] = pin[way, pl.ds(32, 16), :]

    def near_unit(e, carry):
        ffn_one(0, e)
        return carry

    lax.fori_loop(0, 2, near_unit, 0)
    tail = lax.broadcasted_iota(jnp.int32, (16, width), 0)
    for way in (0, 1):
        tails = []
        for e in (0, 1):
            rq[way, pl.ds(e * 16, 16), :] = rc[far - 2, way, pl.ds(e * SLOTS, 16), :]
            tails.append(rc[far - 2, way, pl.ds(e * SLOTS + 16, 16), :].astype(jnp.float32))
        rq[way, pl.ds(32, 16), :] = jnp.where(tail < 4, tails[0], tails[1]).astype(jnp.bfloat16)
    for way in (0, 1):
        near_back(way).start()
    run(rest[len(rest) // 2 :])

    def combine(way, at, step, k, first):
        at_rows = piece(k)
        total = jnp.dot(st[way, at, at_rows, :], rc[at, way], preferred_element_type=jnp.float32)
        if first:
            total = total + jnp.dot(sp[way, at_rows, :], rp[way], preferred_element_type=jnp.float32)
        else:
            total = total + rb[way, step, at_rows, :].astype(jnp.float32)
        rb[way, step, at_rows, :] = total.astype(jnp.bfloat16)

    for way in (0, 1):
        last_back(way).wait_recv()
        near_back(way).wait_recv()
    for k in range(CHUNKS):
        for way in (0, 1):
            combine(way, full - 1, 0, k, True)
        for way in (0, 1):
            sum_copy(way, 0, k).start()

    def bring_back(j, carry):
        for k in range(CHUNKS):
            for way in (0, 1):
                sum_copy(way, j - 1, k).wait_recv()
                combine(way, full - 1 - j, j, k, False)
            for way in (0, 1):
                sum_copy(way, j, k).start()
            if k == 2:

                @pl.when(j == min(6, full - 1))
                def _():
                    shared_ffn()

        return carry

    lax.fori_loop(1, full, bring_back, 0)

    for k in range(CHUNKS):
        at_rows = piece(k)
        total = base[at_rows, :]
        for e in (0, 1):
            total = total + jnp.dot(
                so[at_rows, e * SLOTS : (e + 1) * SLOTS],
                rc[far - 1, 1 - e, pl.ds(e * SLOTS, SLOTS), :],
                preferred_element_type=jnp.float32,
            )
        for way in (0, 1):
            sum_copy(way, full - 1, k).wait_recv()
            total = total + rb[way, full, at_rows, :].astype(jnp.float32)
        out_ref[at_rows, :] = total.astype(jnp.bfloat16)

    def whole(ref, sem):
        return pltpu.make_async_copy(ref, ref, sem)

    for way in (0, 1):

        def drain(i, carry):
            whole(db.at[way, i], d_send.at[way, i]).wait()
            whole(mb.at[way, i], m_send.at[way, i]).wait()
            whole(rb.at[way, i], a_send.at[way, i]).wait()
            return carry

        lax.fori_loop(0, full, drain, 0)
        near_copy(way).wait_send()
        near_back(way).wait_send()
        last_copy(way).wait_send()
        last_back(way).wait_send()
    for a in range(4):
        for k in range(dp - 1):
            weight_copy(a, k).wait_send()
        if a < 2:
            for k in range(dp):
                twin_copy(a, k).wait_send()


def per_device(mesh, tokens, expert_ids, gate_weights, expert_in, expert_out, shared_in, shared_out):
    rows, width = tokens.shape
    hidden = expert_in.shape[2]
    chips, dp = mesh.shape["expert"] // CORES, mesh.shape["dp"]
    far = chips // 2
    full = far - 2
    vmem = pl.BlockSpec(memory_space=pltpu.VMEM)
    hbm = pl.BlockSpec(memory_space=pl.ANY)
    b16, f32, dma = jnp.bfloat16, jnp.float32, pltpu.SemaphoreType.DMA
    return pl.pallas_call(
        functools.partial(kernel, chips, dp),
        out_shape=jax.ShapeDtypeStruct((rows, width), b16),
        in_specs=[vmem, vmem, vmem, hbm, hbm, hbm, hbm],
        out_specs=vmem,
        scratch_shapes=[
            pltpu.VMEM((16, rows), b16),
            pltpu.VMEM((rows, width), b16),
            pltpu.VMEM((2, full, rows, width), b16),
            pltpu.VMEM((2, full, 16, rows), b16),
            pltpu.VMEM((2, full, rows, 2 * SLOTS), b16),
            pltpu.VMEM((2, rows, NEAR + SLOTS), b16),
            pltpu.VMEM((rows, 2 * SLOTS), b16),
            pltpu.VMEM((2, NEAR + SLOTS, width), b16),
            pltpu.VMEM((2, NEAR, width), b16),
            pltpu.VMEM((2, far // 2, 4 * SLOTS, width), b16),
            pltpu.VMEM((far, 2, 2 * SLOTS, width), b16),
            pltpu.VMEM((2, NEAR, width), b16),
            pltpu.VMEM((2, NEAR + SLOTS, width), b16),
            pltpu.VMEM((2, full + 1, rows, width), b16),
            pltpu.VMEM((rows, hidden), b16),
            pltpu.VMEM((rows, width), f32),
            pltpu.VMEM((2, width, hidden), b16),
            pltpu.VMEM((2, hidden, width), b16),
            pltpu.VMEM((width, hidden), b16),
            pltpu.VMEM((hidden, width), b16),
            dma((2, full, CHUNKS)),
            dma((2, full)),
            dma((2, full)),
            dma((2, full)),
            dma((2,)),
            dma((2,)),
            dma((2,)),
            dma((2,)),
            dma((2,)),
            dma((2,)),
            dma((2,)),
            dma((2,)),
            dma((2, full + 1, CHUNKS)),
            dma((2, full)),
            dma((4, dp - 1)),
            dma((4, dp - 1)),
            dma((4,)),
            dma((2, dp)),
            dma((2, dp)),
        ],
        compiler_params=pltpu.CompilerParams(
            collective_id=0, has_side_effects=True, vmem_limit_bytes=67043328
        ),
        name="moe_ring",
    )(tokens, expert_ids.T, gate_weights.T, expert_in, expert_out, shared_in, shared_out)


def solution(mesh):
    placed = (
        P(("sweep", "expert", "dp"), None),
        P(("sweep", "expert", "dp"), None),
        P(("sweep", "expert", "dp"), None),
        P(("sweep", "expert"), "dp", None),
        P(("sweep", "expert"), None, "dp"),
        P(("sweep", "dp"), None),
        P("sweep", "dp"),
    )
    return jax.shard_map(
        functools.partial(per_device, mesh),
        mesh=mesh,
        in_specs=placed,
        out_specs=P(("sweep", "expert", "dp"), None),
        check_vma=False,
    )
```

```python
import functools

import jax
import jax.numpy as jnp
from jax import lax
from jax.experimental import pallas as pl
from jax.experimental.pallas import tpu as pltpu
from jax.sharding import PartitionSpec as P

CORES = 2
SLOTS = 32
NEAR = 48
CHUNKS = 4
FFN_FROM = 8
TILE = 256
MESH = pl.DeviceIdType.MESH


def kernel(
    chips, dp, tok_ref, ids_ref, gates_ref, win_ref, wout_ref, sin_ref, sout_ref, out_ref,
    tk, ob, mo, nb, db, mb, st, sp, so, ps, pq, pin, xb, rc, rq, rp, rb, hb, base, win, wout, sin, sout,
    d_recv, d_send, m_recv, m_send, q_recv, q_send, f_recv, f_send,
    e_recv, e_send, g_recv, g_send, a_recv, a_send,
    w_recv, w_send, w_loc, p_recv, p_send, t_sem, o_sem,
):
    far = chips // 2
    full = far - 2
    pairs = far // 2
    rows, width = tk.shape
    hidden = win.shape[2]
    me = lax.axis_index("expert")
    core = lax.rem(me, CORES)
    chip = me // CORES
    right = lax.rem(chip + 1, chips) * CORES + core
    left = lax.rem(chip + chips - 1, chips) * CORES + core
    partner = chip * CORES + (1 - core)
    xi = lax.axis_index("dp")
    x_up, x_down = lax.rem(xi + 1, dp), lax.rem(xi + dp - 1, dp)
    towards = (right, left)
    right2 = lax.rem(chip + 2, chips) * CORES + core
    left2 = lax.rem(chip + chips - 2, chips) * CORES + core

    barrier = pltpu.get_barrier_semaphore()
    part = rows // CHUNKS

    def piece(k):
        return pl.ds(k * part, part)

    def token_copy(k):
        return pltpu.make_async_copy(tok_ref.at[piece(k)], tk.at[piece(k)], t_sem.at[k])

    def out_copy(k):
        return pltpu.make_async_copy(ob.at[piece(k)], out_ref.at[piece(k)], o_sem.at[k])

    for k in range(CHUNKS):
        token_copy(k).start()
    peers = [{"expert": p} for p in (right, left, partner, right2, left2)] + [{"dp": x_up}, {"dp": x_down}]
    for peer in peers:
        pl.semaphore_signal(barrier, inc=1, device_id=peer, device_id_type=MESH)

    def remote(source, target, send, recv, device):
        return pltpu.make_async_remote_copy(
            src_ref=source, dst_ref=target, send_sem=send, recv_sem=recv,
            device_id=device, device_id_type=MESH,
        )

    def to(way):
        return {"expert": towards[way]}

    def own_copy(way, k):
        return remote(nb.at[piece(k)], db.at[way, 0, piece(k)], d_send.at[way, 0], d_recv.at[way, 0, k], to(way))

    def block_copy(way, at, k):
        return remote(
            db.at[way, at, piece(k)], db.at[way, at + 1, piece(k)], d_send.at[way, at + 1], d_recv.at[way, at + 1, k], to(way)
        )

    def arrived(way, at, k):
        spot = db.at[way, at, piece(k)]
        return remote(spot, spot, d_send.at[way, at], d_recv.at[way, at, k], to(way))

    def meta_arrived(way, at):
        return remote(mb.at[way, at], mb.at[way, at], m_send.at[way, at], m_recv.at[way, at], to(way))

    def own_meta(way):
        return remote(mo, mb.at[way, 0], m_send.at[way, 0], m_recv.at[way, 0], to(way))

    def meta_copy(way, at):
        return remote(mb.at[way, at], mb.at[way, at + 1], m_send.at[way, at + 1], m_recv.at[way, at + 1], to(way))

    def near_copy(way):
        return remote(pq.at[way, pl.ds(0, NEAR)], pin.at[way], q_send.at[way], q_recv.at[way], to(way))

    def last_copy(way):
        return remote(
            pq.at[way, pl.ds(NEAR, SLOTS)],
            xb.at[way, pairs - 1, pl.ds(pl.multiple_of(2 * SLOTS + way * SLOTS, SLOTS), SLOTS)],
            f_send.at[way], f_recv.at[way], {"expert": jnp.where(way == 0, right2, left2)},
        )

    def last_back(way):
        return remote(
            rc.at[far - 1, way, pl.ds(pl.multiple_of(way * SLOTS, SLOTS), SLOTS)],
            rp.at[way, pl.ds(NEAR, SLOTS)],
            e_send.at[way], e_recv.at[way], {"expert": jnp.where(way == 0, left2, right2)},
        )

    def near_back(way):
        return remote(rq.at[way], rp.at[way, pl.ds(0, NEAR)], g_send.at[way], g_recv.at[way], to(1 - way))

    def sum_copy(way, step, k):
        return remote(
            rb.at[way, step, piece(k)], rb.at[way, step + 1, piece(k)], a_send.at[way, step], a_recv.at[way, step + 1, k],
            to(1 - way),
        )

    d_part, f_part = win_ref.shape[1], wout_ref.shape[2]
    shards = (win_ref.at[0], wout_ref.at[0], sin_ref, sout_ref)

    def region(a, shard):
        if a % 2 == 0:
            where = pl.ds(shard * d_part, d_part)
            return win.at[core, where, :] if a == 0 else sin.at[where, :]
        where = pl.ds(pl.multiple_of(shard * f_part, 128), f_part)
        return wout.at[core, :, where] if a == 1 else sout.at[:, where]

    def shard_at(a, k):
        return lax.rem(xi + dp - k, dp) if a % 2 == 0 else lax.rem(xi + k, dp)

    def weight_copy(a, k):
        spot = region(a, shard_at(a, k))
        return remote(
            shards[a] if k == 0 else spot, spot, w_send.at[a, k], w_recv.at[a, k], {"dp": x_up if a % 2 == 0 else x_down}
        )

    def twin_copy(a, k):
        spot = region(a, shard_at(a, k))
        return remote(shards[a] if k == 0 else spot, spot, p_send.at[a, k], p_recv.at[a, k], {"expert": partner})

    def twin_wait(a, k):
        shard = shard_at(a, k)
        if a == 0:
            spot = win.at[1 - core, pl.ds(shard * d_part, d_part), :]
        else:
            spot = wout.at[1 - core, :, pl.ds(pl.multiple_of(shard * f_part, 128), f_part)]
        return remote(spot, spot, p_send.at[a, k], p_recv.at[a, k], {"expert": partner})

    def local_copy(a):
        return pltpu.make_async_copy(shards[a], region(a, xi), w_loc.at[a])

    def norm(k):
        token_copy(k).wait()
        for half in range(part // 16):
            at_rows = pl.ds(k * part + half * 16, 16)
            values = tk[at_rows, :].astype(jnp.float32)
            center = values - jnp.mean(values, axis=-1, keepdims=True)
            spread = jnp.mean(center * center, axis=-1, keepdims=True)
            nb[at_rows, :] = (center * lax.rsqrt(spread + 1e-06)).astype(jnp.bfloat16)

    mo[...] = jnp.concatenate([ids_ref[...].astype(jnp.float32), gates_ref[...]], axis=0).astype(jnp.bfloat16)
    norm(0)
    norm(1)
    pl.semaphore_wait(barrier, len(peers))
    for a in (0, 1):
        weight_copy(a, 0).start()

    for way in (0, 1):
        own_meta(way).start()
    for k in range(CHUNKS):
        for way in (0, 1):
            own_copy(way, k).start()
        if k + 2 < CHUNKS:
            norm(k + 2)
    for a in range(4):
        local_copy(a).start()
    for a in (0, 1):
        twin_copy(a, 0).start()

    def places(meta, experts):
        meta = meta.astype(jnp.float32)
        ids, gates = meta[0:8], meta[8:16]
        match, gate = [], []
        for expert in experts:
            hit = ids == expert.astype(jnp.float32)
            match.append(jnp.sum(jnp.where(hit, 1.0, 0.0), axis=0, keepdims=True))
            gate.append(jnp.sum(jnp.where(hit, gates, 0.0), axis=0, keepdims=True))
        both = jnp.concatenate([jnp.broadcast_to(m, (8, rows)) for m in match], axis=0)
        before = lax.broadcasted_iota(jnp.int32, (rows, rows), 0) < lax.broadcasted_iota(jnp.int32, (rows, rows), 1)
        earlier = jnp.dot(
            both.astype(jnp.bfloat16),
            jnp.where(before, 1.0, 0.0).astype(jnp.bfloat16),
            preferred_element_type=jnp.float32,
        )
        slot = jnp.where(both > 0.5, earlier, -1.0)
        return [slot[8 * i : 8 * i + 8] for i in range(len(experts))], gate

    def row_of(count):
        return lax.broadcasted_iota(jnp.int32, (count, rows), 0).astype(jnp.float32)

    def choose(meta):
        slot, gate = places(meta, (chip * CORES, chip * CORES + 1))
        pick, spread = [], []
        for i in (0, 1):
            here = jnp.concatenate([slot[i]] * (SLOTS // 8), axis=0) == row_of(SLOTS)
            pick.append(jnp.where(here, 1.0, 0.0))
            spread.append(jnp.where(here, jnp.broadcast_to(gate[i], (SLOTS, rows)), 0.0))
        return jnp.concatenate(pick, axis=0).astype(jnp.bfloat16), jnp.concatenate(spread, axis=0).T.astype(jnp.bfloat16)

    def unit_rows(at, way):
        return pl.ds(pl.multiple_of(lax.rem(at, 2) * 2 * SLOTS + way * SLOTS, SLOTS), SLOTS)

    def gather(way, at):
        picked, st[way, at] = choose(mb[way, at])
        for n in range(width // TILE):
            cols = pl.ds(n * TILE, TILE)
            got = jnp.dot(picked, db[way, at, :, cols], preferred_element_type=jnp.float32).astype(jnp.bfloat16)
            for e in (0, 1):
                xb[e, at // 2, unit_rows(at, way), cols] = got[e * SLOTS : e * SLOTS + SLOTS]

    def gather_own():
        picked, spread = choose(mo[...])
        so[...] = spread
        for n in range(width // TILE):
            cols = pl.ds(n * TILE, TILE)
            got = jnp.dot(picked, nb[:, cols], preferred_element_type=jnp.float32).astype(jnp.bfloat16)
            for e in (0, 1):
                xb[e, pairs - 1, pl.ds(2 * SLOTS + (1 - e) * SLOTS, SLOTS), cols] = got[e * SLOTS : e * SLOTS + SLOTS]

    def pack_choice(way):
        ahead = 1 - 2 * way
        near = lax.rem(chip + chips + ahead, chips) * CORES
        last = lax.rem(chip + chips + 2 * ahead, chips) * CORES + way
        meta = mb[way, full - 1]
        slot, gate = places(meta, (near, near + 1))
        slot_last, gate_last = places(meta, (last, last))
        row = row_of(16)
        pick, spread = [], []
        tail_pick, tail_spread = jnp.zeros((16, rows), jnp.float32), jnp.zeros((16, rows), jnp.float32)
        for i in (0, 1):
            where = jnp.concatenate([slot[i], slot[i]], axis=0)
            weight = jnp.broadcast_to(gate[i], (16, rows))
            pick.append(jnp.where(where == row, 1.0, 0.0))
            spread.append(jnp.where(where == row, weight, 0.0))
            inside = jnp.where((row >= 4 * i) & (row < 4 * i + 4), row + (16 - 4 * i), -2.0)
            tail_pick = jnp.where(where == inside, 1.0, tail_pick)
            tail_spread = jnp.where(where == inside, weight, tail_spread)
        here = jnp.concatenate([slot_last[0]] * (SLOTS // 8), axis=0) == row_of(SLOTS)
        pick += [tail_pick, jnp.where(here, 1.0, 0.0)]
        spread += [tail_spread, jnp.where(here, jnp.broadcast_to(gate_last[0], (SLOTS, rows)), 0.0)]
        ps[way] = jnp.concatenate(pick, axis=0).astype(jnp.bfloat16)
        filler = [jnp.zeros((rows - NEAR - SLOTS, rows), jnp.float32)]
        sp[way] = jnp.concatenate(spread + filler, axis=0).T[:, : NEAR + SLOTS].astype(jnp.bfloat16)

    def pack(way):
        for n in range(width // TILE):
            cols = pl.ds(n * TILE, TILE)
            pq[way, :, cols] = jnp.dot(
                ps[way], db[way, full - 1, :, cols], preferred_element_type=jnp.float32
            ).astype(jnp.bfloat16)

    def two_dots(count, source, first, second, store):
        for n in range(hidden // TILE):
            cols = pl.ds(n * TILE, TILE)
            pre = jnp.dot(source(), first(cols), preferred_element_type=jnp.float32)
            hb[:count, cols] = jax.nn.gelu(pre, approximate=True).astype(jnp.bfloat16)
        for n in range(width // TILE):
            cols = pl.ds(n * TILE, TILE)
            store(cols, jnp.dot(hb[:count], second(cols), preferred_element_type=jnp.float32))

    def ffn(call):
        pair, e = call // 2, lax.rem(call, 2)

        def store(cols, result):
            result = result.astype(jnp.bfloat16)
            for h in (0, 1):
                for way in (0, 1):
                    lo = (2 * h + way) * SLOTS
                    rc[2 * pair + h, way, pl.ds(pl.multiple_of(e * SLOTS, SLOTS), SLOTS), cols] = result[lo : lo + SLOTS]

        two_dots(4 * SLOTS, lambda: xb[e, pair], lambda cols: win[e, :, cols], lambda cols: wout[e, :, cols], store)

    def ffn_one(h, e):
        def store(cols, result):
            result = result.astype(jnp.bfloat16)
            for way in (0, 1):
                rc[far - 2 + h, way, pl.ds(pl.multiple_of(e * SLOTS, SLOTS), SLOTS), cols] = result[
                    way * SLOTS : (way + 1) * SLOTS
                ]

        source = pl.ds(2 * SLOTS * h, 2 * SLOTS)
        two_dots(
            2 * SLOTS, lambda: xb[e, pairs - 1, source, :], lambda cols: win[e, :, cols], lambda cols: wout[e, :, cols], store
        )

    def shared_ffn():
        def store(cols, result):
            base[:, cols] = tk[:, cols].astype(jnp.float32) + result

        two_dots(rows, lambda: nb[...], lambda cols: sin[:, cols], lambda cols: sout[:, cols], store)

    def calls_by(step_index):
        done = jnp.minimum(2 * (step_index // 2), 2 * (step_index + 1 - FFN_FROM))
        return jnp.maximum(done, 0)

    def dispatch(i, carry):
        lo, hi = calls_by(i - 1), calls_by(i)
        lo = jnp.where(i == 0, 0, lo)
        for k in range(CHUNKS):
            for way in (0, 1):
                arrived(way, i, k).wait_recv()

                @pl.when(i + 1 < full)
                def _():
                    block_copy(way, i, k).start()

                if k == 0:
                    meta_arrived(way, i).wait_recv()

                    @pl.when(i + 1 < full)
                    def _():
                        meta_copy(way, i).start()

            if k == 0:

                @pl.when(i == 0)
                def _():
                    gather_own()

                @pl.when(i > 0)
                def _():
                    gather(0, i - 1)

            if k == 1:

                @pl.when(i > 0)
                def _():
                    gather(1, i - 1)

            if k == 2:

                @pl.when(i == full - 1)
                def _():
                    pack_choice(0)
                    pack_choice(1)

            if k >= 2:

                @pl.when(lo + (k - 2) < hi)
                def _():
                    ffn(lo + (k - 2))

            if k == 3:

                for hop in range(dp - 1):
                    for first, pair in ((0, (0, 1)), (2 * dp - 2, (2, 3))):

                        @pl.when(i == min(first + 2 * hop + 1, full - 1))
                        def _():
                            for a in pair:
                                weight_copy(a, hop).wait_recv()
                                if hop + 1 < dp - 1:
                                    weight_copy(a, hop + 1).start()
                                if a < 2:
                                    twin_copy(a, hop + 1).start()
                                if hop == dp - 2:
                                    local_copy(a).wait()
                                    if a < 2:
                                        weight_copy(a + 2, 0).start()
                                        for j in range(dp):
                                            twin_wait(a, j).wait_recv()

        return carry

    lax.fori_loop(0, full, dispatch, 0)
    for way in (0, 1):
        pack(way)
    for way in (0, 1):
        last_copy(way).start()
        near_copy(way).start()
    for way in (0, 1):
        gather(way, full - 1)
    started = max(0, min(2 * ((full - 1) // 2), 2 * (full - FFN_FROM)))
    rest = list(range(started, 2 * (pairs - 1)))

    def run(calls):
        if calls:

            def body(c, carry):
                ffn(c)
                return carry

            lax.fori_loop(calls[0], calls[-1] + 1, body, 0)

    run(rest[: len(rest) // 2])

    def last_unit(e, carry):
        last_copy(e).wait_recv()
        ffn_one(1, e)
        last_back(e).start()
        return carry

    lax.fori_loop(0, 2, last_unit, 0)
    for way in (0, 1):
        near_copy(way).wait_recv()
        for e in (0, 1):
            xb[e, pairs - 1, pl.ds(way * SLOTS, 16), :] = pin[way, pl.ds(e * 16, 16), :]
            xb[e, pairs - 1, pl.ds(way * SLOTS + 16, 16), :] = pin[way, pl.ds(32, 16), :]

    def near_unit(e, carry):
        ffn_one(0, e)
        return carry

    lax.fori_loop(0, 2, near_unit, 0)
    tail = lax.broadcasted_iota(jnp.int32, (16, width), 0)
    for way in (0, 1):
        tails = []
        for e in (0, 1):
            rq[way, pl.ds(e * 16, 16), :] = rc[far - 2, way, pl.ds(e * SLOTS, 16), :]
            tails.append(rc[far - 2, way, pl.ds(e * SLOTS + 16, 16), :].astype(jnp.float32))
        rq[way, pl.ds(32, 16), :] = jnp.where(tail < 4, tails[0], tails[1]).astype(jnp.bfloat16)
    for way in (0, 1):
        near_back(way).start()
    run(rest[len(rest) // 2 :])

    def combine(way, at, step, k, first):
        at_rows = piece(k)
        total = jnp.dot(st[way, at, at_rows, :], rc[at, way], preferred_element_type=jnp.float32)
        if first:
            total = total + jnp.dot(sp[way, at_rows, :], rp[way], preferred_element_type=jnp.float32)
        else:
            total = total + rb[way, step, at_rows, :].astype(jnp.float32)
        rb[way, step, at_rows, :] = total.astype(jnp.bfloat16)

    for way in (0, 1):
        last_back(way).wait_recv()
        near_back(way).wait_recv()
    for k in range(CHUNKS):
        for way in (0, 1):
            combine(way, full - 1, 0, k, True)
        for way in (0, 1):
            sum_copy(way, 0, k).start()

    def bring_back(j, carry):
        for k in range(CHUNKS):
            for way in (0, 1):
                sum_copy(way, j - 1, k).wait_recv()
                combine(way, full - 1 - j, j, k, False)
            for way in (0, 1):
                sum_copy(way, j, k).start()
            if k == 2:

                @pl.when(j == min(6, full - 1))
                def _():
                    shared_ffn()

        return carry

    lax.fori_loop(1, full, bring_back, 0)

    for k in range(CHUNKS):
        at_rows = piece(k)
        total = base[at_rows, :]
        for e in (0, 1):
            total = total + jnp.dot(
                so[at_rows, e * SLOTS : (e + 1) * SLOTS],
                rc[far - 1, 1 - e, pl.ds(e * SLOTS, SLOTS), :],
                preferred_element_type=jnp.float32,
            )
        for way in (0, 1):
            sum_copy(way, full - 1, k).wait_recv()
            total = total + rb[way, full, at_rows, :].astype(jnp.float32)
        ob[at_rows, :] = total.astype(jnp.bfloat16)
        out_copy(k).start()

    for k in range(CHUNKS):
        out_copy(k).wait()
    def whole(ref, sem):
        return pltpu.make_async_copy(ref, ref, sem)

    for way in (0, 1):

        def drain(i, carry):
            whole(db.at[way, i], d_send.at[way, i]).wait()
            whole(mb.at[way, i], m_send.at[way, i]).wait()
            whole(rb.at[way, i], a_send.at[way, i]).wait()
            return carry

        lax.fori_loop(0, full, drain, 0)
        near_copy(way).wait_send()
        near_back(way).wait_send()
        last_copy(way).wait_send()
        last_back(way).wait_send()
    for a in range(4):
        for k in range(dp - 1):
            weight_copy(a, k).wait_send()
        if a < 2:
            for k in range(dp):
                twin_copy(a, k).wait_send()


def per_device(mesh, tokens, expert_ids, gate_weights, expert_in, expert_out, shared_in, shared_out):
    rows, width = tokens.shape
    hidden = expert_in.shape[2]
    chips, dp = mesh.shape["expert"] // CORES, mesh.shape["dp"]
    far = chips // 2
    full = far - 2
    vmem = pl.BlockSpec(memory_space=pltpu.VMEM)
    hbm = pl.BlockSpec(memory_space=pl.ANY)
    b16, f32, dma = jnp.bfloat16, jnp.float32, pltpu.SemaphoreType.DMA
    return pl.pallas_call(
        functools.partial(kernel, chips, dp),
        out_shape=jax.ShapeDtypeStruct((rows, width), b16),
        in_specs=[hbm, vmem, vmem, hbm, hbm, hbm, hbm],
        out_specs=hbm,
        scratch_shapes=[
            pltpu.VMEM((rows, width), b16),
            pltpu.VMEM((rows, width), b16),
            pltpu.VMEM((16, rows), b16),
            pltpu.VMEM((rows, width), b16),
            pltpu.VMEM((2, full, rows, width), b16),
            pltpu.VMEM((2, full, 16, rows), b16),
            pltpu.VMEM((2, full, rows, 2 * SLOTS), b16),
            pltpu.VMEM((2, rows, NEAR + SLOTS), b16),
            pltpu.VMEM((rows, 2 * SLOTS), b16),
            pltpu.VMEM((2, NEAR + SLOTS, rows), b16),
            pltpu.VMEM((2, NEAR + SLOTS, width), b16),
            pltpu.VMEM((2, NEAR, width), b16),
            pltpu.VMEM((2, far // 2, 4 * SLOTS, width), b16),
            pltpu.VMEM((far, 2, 2 * SLOTS, width), b16),
            pltpu.VMEM((2, NEAR, width), b16),
            pltpu.VMEM((2, NEAR + SLOTS, width), b16),
            pltpu.VMEM((2, full + 1, rows, width), b16),
            pltpu.VMEM((rows, hidden), b16),
            pltpu.VMEM((rows, width), f32),
            pltpu.VMEM((2, width, hidden), b16),
            pltpu.VMEM((2, hidden, width), b16),
            pltpu.VMEM((width, hidden), b16),
            pltpu.VMEM((hidden, width), b16),
            dma((2, full, CHUNKS)),
            dma((2, full)),
            dma((2, full)),
            dma((2, full)),
            dma((2,)),
            dma((2,)),
            dma((2,)),
            dma((2,)),
            dma((2,)),
            dma((2,)),
            dma((2,)),
            dma((2,)),
            dma((2, full + 1, CHUNKS)),
            dma((2, full)),
            dma((4, dp - 1)),
            dma((4, dp - 1)),
            dma((4,)),
            dma((2, dp)),
            dma((2, dp)),
            dma((CHUNKS,)),
            dma((CHUNKS,)),
        ],
        compiler_params=pltpu.CompilerParams(
            collective_id=0, has_side_effects=True, vmem_limit_bytes=67043328
        ),
        name="moe_ring",
    )(tokens, expert_ids.T, gate_weights.T, expert_in, expert_out, shared_in, shared_out)


def solution(mesh):
    placed = (
        P(("sweep", "expert", "dp"), None),
        P(("sweep", "expert", "dp"), None),
        P(("sweep", "expert", "dp"), None),
        P(("sweep", "expert"), "dp", None),
        P(("sweep", "expert"), None, "dp"),
        P(("sweep", "dp"), None),
        P("sweep", "dp"),
    )
    return jax.shard_map(
        functools.partial(per_device, mesh),
        mesh=mesh,
        in_specs=placed,
        out_specs=P(("sweep", "expert", "dp"), None),
        check_vma=False,
    )
```
